256 devices in a mesh: ep: 64 (over z, x, core), tp: 4 (over y).
Axes of the slice: x: 4, y: 4, z: 8, core: 2. Of those that a mesh axis runs over, the one named last changes fastest.
Arguments:
- tokens: bfloat16 [8192, 4096], P('ep', 'tp'), may hold values from -6 to 6
- expert_ids: int32 [8192, 2], P('ep'), may hold values from 0 to 7, all different within a row; in each aligned block of 128 rows (0 to 127, 128 to 255, ...) at most 40 rows name the same one
- gates: float32 [8192, 2], P('ep'), may hold values from 0.1 to 1
- gate_weight: bfloat16 [4096, 57344], P('tp', 'ep'), may hold values from -0.09375 to 0.09375
- up_weight: bfloat16 [4096, 57344], P('tp', 'ep'), may hold values from -0.09375 to 0.09375
- down_weight: bfloat16 [57344, 4096], P('ep', 'tp'), may hold values from -0.0625 to 0.0625
Outputs:
- mixed: bfloat16 [8192, 4096], P('ep', 'tp')
- expert_counts: float32 [8], replicated
- aux_loss: float32 [], replicated
The draws below stay inside these ranges and needn't reach their ends.
Inputs may be any that keep to these rules, and one draw needn't show every extreme that they name: `expert_ids`: each token names 2 different experts. Among the tokens of one index of ep no expert is named more than 40 times, and in every draw some expert is named exactly 40 times by some index's tokens; every expert is named somewhere.
All inputs are finite; a program needn't handle non-finite values.
Results may differ from the reference program's by a relative error of at most 0.008.
Values may be sent and summed in bfloat16 or wider, within the bound.
No kernel may reach another device: no remote copies, remote signals or barrier semaphores. Data moves between devices by JAX's collectives and lax.ppermute only.
A program may use at most 128 MiB of HBM per device.

```python
import math
import jax
import jax.numpy as jnp
import numpy as np
from jax import lax

D = 4096
FF = 7168
EXPERTS = 8
TOP = 2
TOK_DEV = 128
CAP = 40
REPLICAS = 8
TOKENS = 8192
N_EP = 64


def block_scale(stream_key, dims, shards, smallest, high):
    def one(axis_at, parts):
        steps = jax.random.uniform(jax.random.fold_in(jax.random.fold_in(stream_key, 6), axis_at), (parts,), jnp.float32, smallest / len(shards), high / len(shards))
        return jnp.repeat(jnp.exp(steps), dims[axis_at] // parts).reshape((-1,) + (1,) * (len(dims) - axis_at - 1))

    level = one(*shards[0])
    for cut in shards[1:]:
        level = level * one(*cut)
    return level


def routed_block(stream_key, own, number, rows, count, top, bound, lean):
    ranking = jax.random.permutation(stream_key, count)
    crowded, ordinary = load_shares(count, rows * top, bound, lean, True), load_shares(count, rows * top, bound, lean, False)
    places = jnp.arange(count)

    def named(lengths, offset_by):
        used = int((lengths > 0).sum())
        fixed = max(1, used // 4)
        moved = fixed + (places - fixed + offset_by * (used - fixed)) % max(1, count - fixed)
        return jnp.zeros((count,), jnp.int32).at[ranking[jnp.where(places < fixed, places, moved)]].set(jnp.asarray(lengths, jnp.int32))

    lengths = jnp.where(number % 4 == 0, named(crowded, number // 4), named(ordinary, number - number // 4 - 1))
    mixed = jax.random.permutation(jax.random.fold_in(own, 3), count)
    source_of, taker = mixed[0:count // 2 * 2:2], mixed[1:count // 2 * 2:2]
    room = jnp.minimum(lengths[source_of] - 1, bound - lengths[taker]) // 2
    room = jnp.where((source_of == ranking[0]) | (taker == ranking[0]) | (lengths[taker] == 0), 0, jnp.maximum(room, 0))
    moved = jax.random.randint(jax.random.fold_in(own, 4), (count // 2,), 0, 1 << 20) % (room + 1)
    lengths = lengths.at[source_of].add(-moved).at[taker].add(moved)
    members = jnp.searchsorted(jnp.cumsum(lengths), jnp.arange(rows * top), side="right").astype(jnp.int32)
    table = members.reshape(top, rows).T
    table = table[jax.random.permutation(jax.random.fold_in(own, 1), rows)]
    offset_by = jax.random.randint(jax.random.fold_in(own, 2), (rows, 1), 0, top)
    return jnp.take_along_axis(table, (jnp.arange(top)[None, :] + offset_by) % top, axis=1)


def load_shares(count, total, limit, slope, full):
    loads = [(1 << 20) // math.isqrt(standing ** slope) + 1 for standing in range(1, count + 1)]
    largest = limit if full else min(limit, max(-(-total // count), total * loads[0] // sum(loads)))
    least = 1 if total - largest >= count - 1 else 0
    given, spare = [largest] + [least] * (count - 1), total - largest - least * (count - 1)
    while spare > 0:
        candidates = [i for i in range(1, count) if given[i] < largest] or [i for i in range(1, count) if given[i] < limit]
        pool, left = sum([loads[i] for i in candidates]), spare
        for i in candidates:
            extra = min(limit - given[i], max(1, left * loads[i] // pool), spare)
            given[i] = given[i] + extra
            spare = spare - extra
    return np.array(given)


def normal_values(stream_key, extent, scale, limit, cuts=(), held_as=jnp.bfloat16):
    array = jax.random.normal(stream_key, extent, jnp.float32) * scale
    if len(cuts) > 0:
        array = block_scale(stream_key, extent, cuts, -0.22, 0.18) * array
    return jnp.clip(array, min=-limit, max=limit).astype(held_as)


def setup_inputs(seed: int = 0) -> dict:
    key_of = jax.random.split(jax.random.key(seed), 7)
    tokens = normal_values(key_of[0], (TOKENS, D), 1.0, 6.0, ((0, 64), (1, 4)))
    expert_ids_keys = jax.random.split(jax.random.fold_in(key_of[1], 1), TOKENS // TOK_DEV)
    expert_ids_turns = jax.random.permutation(jax.random.fold_in(key_of[1], 3), TOKENS // TOK_DEV)
    expert_ids = jax.vmap(lambda own, number: routed_block(jax.random.fold_in(key_of[1], 2), own, number, TOK_DEV, EXPERTS, TOP, CAP, 2))(expert_ids_keys, expert_ids_turns).reshape((TOKENS, TOP))
    gates = jnp.clip(0.1 + 0.9 * jax.random.uniform(key_of[2], (TOKENS, TOP), jnp.float32) ** block_scale(key_of[2], (TOKENS, TOP), ((0, 64),), -0.2, 0.2), 0.1, 1.0)
    gate_weight = normal_values(key_of[3], (D, EXPERTS * FF), D ** -0.5, 0.09375, ((0, 4), (1, 64)))
    up_weight = normal_values(key_of[4], (D, EXPERTS * FF), D ** -0.5, 0.09375, ((0, 4), (1, 64)))
    down_weight = normal_values(key_of[5], (EXPERTS * FF, D), FF ** -0.5, 0.0625, ((0, 64), (1, 4)))
    return dict(tokens=tokens, expert_ids=expert_ids, gates=gates, gate_weight=gate_weight, up_weight=up_weight, down_weight=down_weight)


def reference(tokens, expert_ids, gates, gate_weight, up_weight, down_weight):
    assign = TOK_DEV * TOP
    ids = expert_ids.reshape(N_EP, assign)
    onehot = (ids[:, :, None] == jnp.arange(EXPERTS, dtype=jnp.int32)[None, None, :]).astype(jnp.int32)
    before = jnp.cumsum(onehot, axis=1) - onehot
    slot = jnp.sum(before * onehot, axis=2)
    target = ids * CAP + slot
    place = (target[:, :, None] == jnp.arange(EXPERTS * CAP, dtype=jnp.int32)[None, None, :]).astype(jnp.float32)
    blocks = jnp.repeat(tokens.reshape(N_EP, TOK_DEV, D), TOP, axis=1).astype(jnp.float32)
    dispatched = jnp.einsum("jas,jad->jsd", place, blocks, precision=lax.Precision.HIGHEST).astype(jnp.bfloat16)
    per_expert = dispatched.reshape(N_EP, EXPERTS, CAP, D).transpose(1, 0, 2, 3).reshape(EXPERTS, N_EP * CAP, D)
    gate_cols = gate_weight.reshape(D, EXPERTS, FF).transpose(1, 0, 2)
    up_cols = up_weight.reshape(D, EXPERTS, FF).transpose(1, 0, 2)
    down_rows = down_weight.reshape(EXPERTS, FF, D)

    def expert(operands):
        rows, gate_e, up_e, down_e = operands
        gate = jnp.dot(rows, gate_e, preferred_element_type=jnp.float32)
        upper = jnp.dot(rows, up_e, preferred_element_type=jnp.float32)
        hidden = (jax.nn.silu(gate) * upper).astype(jnp.bfloat16)
        pieces = hidden.reshape(-1, REPLICAS, FF // REPLICAS).astype(jnp.float32)
        downs = down_e.reshape(REPLICAS, FF // REPLICAS, D).astype(jnp.float32)
        partial_value = jnp.einsum("nrf,rfd->rnd", pieces, downs).astype(jnp.bfloat16)
        partial_value = lax.optimization_barrier(partial_value)
        return jnp.sum(partial_value.astype(jnp.float32), axis=0)

    outputs = lax.map(expert, (per_expert, gate_cols, up_cols, down_rows))
    results = outputs.reshape(EXPERTS, N_EP, CAP, D).transpose(1, 0, 2, 3).reshape(N_EP, EXPERTS * CAP, D)
    weighted = place * gates.reshape(N_EP, assign)[:, :, None]
    combine = weighted.reshape(N_EP, TOK_DEV, TOP, EXPERTS * CAP).sum(axis=2)
    mixed = jnp.einsum("jts,jsd->jtd", combine, results, precision=lax.Precision.HIGHEST)
    mixed = mixed.reshape(TOKENS, D).astype(jnp.bfloat16)
    counts = jnp.sum(onehot, axis=(0, 1)).astype(jnp.float32)
    totals = jnp.sum(onehot.astype(jnp.float32) * gates.reshape(N_EP, assign)[:, :, None], axis=(0, 1))
    aux_loss = EXPERTS * jnp.sum(counts / (TOP * TOKENS) * (totals / TOKENS))
    return mixed, counts, aux_loss
```

```python
import jax
import jax.numpy as jnp
from jax import lax
from jax.sharding import PartitionSpec as P

EXPERTS = 8
TOP = 2
CAP = 40
NZ, NX, NC, NY = 8, 4, 2, 4
BF16 = jnp.bfloat16
F32 = jnp.float32


def device_index(z, x, c, y):
    return (((z % NZ) * NX + x % NX) * NC + c) * NY + y % NY


def move(value, to):
    pairs = []
    for z in range(NZ):
        for x in range(NX):
            for c in range(NC):
                for y in range(NY):
                    pairs.append((device_index(z, x, c, y), device_index(*to(z, x, c, y))))
    return lax.ppermute(value, ("ep", "tp"), pairs)


def along_y(value, by):
    return move(value, lambda z, x, c, y: (z, x, c, y + by))


def along_x(value, by):
    return move(value, lambda z, x, c, y: (z, x + by, c, y))


def other_core(value):
    return move(value, lambda z, x, c, y: (z, x, 1 - c, y))


def dot(a, b):
    return jnp.dot(a, b, preferred_element_type=F32)


def total_over_ep(value):
    for bit in (1, 2, 4, 8, 16, 32):
        value = value + lax.ppermute(value, "ep", [(s, s ^ bit) for s in range(NZ * NX * NC)])
    return value


def gather_down(down):
    half = down.shape[0] // 2
    before = along_y(down, 1)
    after = along_y(down, -1)
    opposite = jnp.concatenate([along_y(before[:half], 1), along_y(after[half:], -1)], axis=0)
    return jnp.concatenate([down, after, opposite, before], axis=1)


def per_device(tokens, expert_ids, gates, gate_weight, up_weight, down_weight):
    count_tok, quarter = tokens.shape
    ep = lax.axis_index("ep")
    z, y = ep // (NX * NC), lax.axis_index("tp")
    down_all = gather_down(down_weight)

    flat_ids = expert_ids.reshape(-1)
    onehot = (flat_ids[:, None] == jnp.arange(EXPERTS, dtype=jnp.int32)[None, :]).astype(jnp.int32)
    before = jnp.cumsum(onehot, axis=0) - onehot
    slot = jnp.sum(before * onehot, axis=1)
    ahead = (flat_ids - z) % NZ
    place = (ahead % 2) * NY + (ahead // 2 - y) % NY
    target = (place * CAP + slot).reshape(count_tok, TOP)
    matches = target[:, :, None] == jnp.arange(EXPERTS * CAP, dtype=jnp.int32)[None, None, :]
    combine = jnp.sum(jnp.where(matches, gates[:, :, None], 0.0), axis=1)
    selector = jnp.any(matches, axis=1).astype(BF16)

    arrived = {}
    for p in (2, 1, 3, 0):
        for i in range(2):
            at = (i * NY + p) * CAP
            rows = lax.dot_general(
                selector[:, at : at + CAP], tokens, (((0,), (0,)), ((), ())), preferred_element_type=F32
            ).astype(BF16)
            arrived[i, p] = move(rows, lambda z, x, c, y: (z + 2 * ((y + p) % NY) + i, x, c, y))
    own = jnp.concatenate([arrived[i, p] for i in range(2) for p in range(NY)], axis=0)
    row_x = jnp.stack([own] + [along_x(own, j) for j in (1, 2, 3)])
    both = jnp.stack([row_x, other_core(row_x)])
    both = both.reshape(NC, NX, 2, NY, CAP, quarter)

    def rows_of(i, p):
        return both[:, :, i, p].reshape(NC * NX * CAP, quarter)

    first = {}
    for i in range(2):
        x_rows = rows_of(i, 2)
        first[i] = (
            along_y(dot(x_rows, gate_weight).astype(BF16), 1),
            along_y(dot(x_rows, up_weight).astype(BF16), -1),
        )
    second = {}
    for i in range(2):
        gate_in, up_in = first[i]
        x_rows = rows_of(i, 1)
        right = jnp.concatenate(
            [(dot(x_rows, gate_weight) + gate_in.astype(F32)).astype(BF16), dot(x_rows, up_weight).astype(BF16)], axis=0
        )
        x_rows = rows_of(i, 3)
        left = jnp.concatenate(
            [dot(x_rows, gate_weight).astype(BF16), (dot(x_rows, up_weight) + up_in.astype(F32)).astype(BF16)], axis=0
        )
        second[i] = (along_y(right, 1), along_y(left, -1))

    mixed = None
    combine = combine.reshape(count_tok, 2, NY * CAP)
    for i in range(2):
        x_rows = rows_of(i, 0)
        count = x_rows.shape[0]
        from_left, from_right = second[i]
        gate = dot(x_rows, gate_weight) + from_left[:count].astype(F32) + from_right[:count].astype(F32)
        up = dot(x_rows, up_weight) + from_left[count:].astype(F32) + from_right[count:].astype(F32)
        hidden = (jax.nn.silu(gate) * up).astype(BF16)
        half = count // 2
        sent = other_core(dot(hidden[half:], down_all).astype(BF16))
        chip = (dot(hidden[:half], down_all) + sent.astype(F32)).astype(BF16)
        total = chip[:CAP].astype(F32)
        for j in (1, 2, 3):
            total = total + along_x(chip[j * CAP : (j + 1) * CAP], -j).astype(F32)
        total = total.astype(BF16)
        home = [None] * NY
        for q in range(NY):
            home[-q % NY] = move(
                total[:, q * quarter : (q + 1) * quarter],
                lambda z, x, c, y: (z - (2 * y + i), x, c, y + q),
            )
        part = jnp.dot(
            combine[:, i],
            jnp.concatenate(home, axis=0).astype(F32),
            precision=lax.Precision.HIGHEST,
            preferred_element_type=F32,
        )
        mixed = part if mixed is None else mixed + part

    counts = jnp.sum(onehot, axis=0).astype(F32)
    totals = jnp.sum(onehot.astype(F32) * gates.reshape(-1)[:, None], axis=0)
    both_totals = total_over_ep(jnp.concatenate([counts, totals]))
    counts, totals = both_totals[:EXPERTS], both_totals[EXPERTS:]
    tokens_all = count_tok * NZ * NX * NC
    aux_loss = EXPERTS * jnp.sum(counts / (TOP * tokens_all) * (totals / tokens_all))
    return (mixed.astype(BF16), counts, aux_loss)


def solution(mesh):
    placed = (
        P("ep", "tp"),
        P("ep", None),
        P("ep", None),
        P("tp", "ep"),
        P("tp", "ep"),
        P("ep", "tp"),
    )
    return jax.shard_map(
        per_device, mesh=mesh, in_specs=placed, out_specs=(P("ep", "tp"), P(), P()), check_vma=False
    )
```
